64 devices in a mesh: dp: 4 (over x, y), sp: 16 (over z, core).
Axes of the slice: x: 2, y: 2, z: 8, core: 2. Of those that a mesh axis runs over, the one named last changes fastest.
The devices are a block of a 4x4x8 slice.
Arguments:
- q: bfloat16 [128, 64, 128], P('dp'), parts along dimension 0
- k: bfloat16 [128, 8192, 8, 128], P('dp', 'sp'), parts along dimension 0
- v: bfloat16 [128, 8192, 8, 128], P('dp', 'sp'), parts along dimension 0
Outputs:
- q: bfloat16 [128, 64, 128], P('dp'), parts along dimension 0
There are 4 independent parts. The reference program is written for one: setup_inputs(seed, part) draws one part's arguments, and reference() takes and returns one part's arrays. A program takes and returns all parts, laid end to end along the dimension named above; each array names one.
All inputs are finite; a program needn't handle non-finite values.
Results may differ from the reference program's by a relative error of at most 0.012.
Values are sent between devices in bfloat16 or wider.
A program may use at most 768 MiB of HBM per device.

```python
import jax
import jax.numpy as jnp

BATCH = 32
CACHE = 8192
HEADS = 64
KV_HEADS = 8
HEAD = 128


def setup_inputs(seed: int = 0, part: int = 0) -> dict:
    kq, kk, kv = (jax.random.fold_in(k, part) for k in jax.random.split(jax.random.key(seed), 3))
    return {
        "q": (3 * jax.random.normal(kq, (BATCH, HEADS, HEAD), jnp.float32)).astype(jnp.bfloat16),
        "k": jax.random.normal(kk, (BATCH, CACHE, KV_HEADS, HEAD), jnp.float32).astype(jnp.bfloat16),
        "v": jax.random.normal(kv, (BATCH, CACHE, KV_HEADS, HEAD), jnp.float32).astype(jnp.bfloat16),
    }


def einsum(form, a, b):
    return jnp.einsum(form, a.astype(jnp.float32), b.astype(jnp.float32))


def reference(q, k, v):
    grouped = q.reshape(BATCH, KV_HEADS, -1, HEAD)
    scores = einsum("bgsd,bugd->bgsu", grouped, k) * HEAD**-0.5
    weights = jax.nn.softmax(scores, -1).astype(jnp.bfloat16)
    return einsum("bgsu,bugd->bgsd", weights, v).astype(jnp.bfloat16).reshape(BATCH, HEADS, HEAD)
```

```python
import functools

import jax
import jax.numpy as jnp
from jax import lax
from jax.experimental import pallas as pl
from jax.experimental.pallas import tpu as pltpu
from jax.sharding import PartitionSpec as P

SLOTS = 8
BLOCK = 512
CORES = 2
SUB = 8
LOG2E = 1.4426950408889634


def chunks_of(n, unit):
    sizes = [4 * unit] * (n // (4 * unit) - 1) + [2 * unit, unit, unit]
    assert sum(sizes) == n
    return [(sum(sizes[:i]), g) for i, g in enumerate(sizes)]


def kernel(size, chunks, scale, heads, q_ref, k_hbm, v_hbm, o_ref, kbuf, vbuf, sbuf, pbuf, send, stat, cols, *rest):
    nc = len(chunks)
    recv, rstat = rest[:nc], rest[nc : 2 * nc]
    ksem, vsem, sems = rest[2 * nc :]
    PART_OUT, PART_IN, STAT_OUT, STAT_IN, RES_OUT, RES_IN, PASS_OUT, PASS_IN = range(8)
    n, nq, d = q_ref.shape
    rows = k_hbm.shape[1]
    half = rows // 2
    nblk = half // BLOCK
    per = nq // SUB
    c2 = scale * LOG2E
    me = lax.axis_index("sp")
    zs = size // CORES
    core, z = lax.rem(me, CORES), me // CORES

    def owner(j):
        return lax.rem(j, CORES) * zs + j // CORES

    barrier = pltpu.get_barrier_semaphore()
    for i in range(1, size):
        pl.semaphore_signal(barrier, inc=1, device_id={"sp": lax.rem(me + i, size)}, device_id_type=pl.DeviceIdType.MESH)

    def kcopy(s):
        return pltpu.make_async_copy(k_hbm.at[s], kbuf.at[lax.rem(s, SLOTS)], ksem.at[lax.rem(s, SLOTS)])

    def vcopy(s):
        return pltpu.make_async_copy(v_hbm.at[s], vbuf.at[lax.rem(s, SLOTS)], vsem.at[lax.rem(s, SLOTS)])

    for s in range(SLOTS):
        kcopy(s).start()
        vcopy(s).start()

    row = lax.broadcasted_iota(jnp.int32, (heads, 2 * nq), 0)
    lane = lax.broadcasted_iota(jnp.int32, (heads, 2 * nq), 1)
    keep = row == lax.rem(lane, nq) // (nq // heads)
    first = lax.broadcasted_iota(jnp.int32, (1, 2 * nq), 1) < nq

    def scores(s, b, w, m):
        slot = lax.rem(s, SLOTS)
        k0 = kbuf[slot, pl.ds(b * BLOCK, BLOCK), :]
        k1 = kbuf[slot, pl.ds(half + b * BLOCK, BLOCK), :]
        x = lax.dot_general(jnp.concatenate([k0, k1], 1), w, (((1,), (1,)), ((), ())), preferred_element_type=jnp.float32)
        x = jnp.where(keep[None], x.reshape(BLOCK // heads, heads, 2 * nq), -jnp.inf)
        sbuf[pl.ds(b * BLOCK, BLOCK), :] = x.reshape(BLOCK, 2 * nq)
        return jnp.maximum(m, jnp.max(x, 0))

    def weights(b, mc, l):
        p = jnp.exp2(sbuf[pl.ds(b * BLOCK, BLOCK), :] * c2 - mc)
        pbuf[:, pl.ds(b * BLOCK, BLOCK)] = p.astype(jnp.bfloat16).T
        return l + jnp.sum(p.reshape(BLOCK // heads, heads, 2 * nq), 0)

    def values(s, b, acc):
        slot = lax.rem(s, SLOTS)
        at = pl.ds(b * BLOCK, BLOCK)
        acc = acc + jnp.dot(pbuf[:nq, at], vbuf[slot, at, :], preferred_element_type=jnp.float32)
        return acc + jnp.dot(pbuf[nq:, at], vbuf[slot, pl.ds(half + b * BLOCK, BLOCK), :], preferred_element_type=jnp.float32)

    def fold(x, op, reduce):
        x = reduce(x, 0, keepdims=True)
        return op(x, pltpu.roll(x, nq, 1))

    def stage(s, state, which):
        m8, l8, m2 = state
        m = jnp.full((heads, 2 * nq), -jnp.inf, jnp.float32)
        l = jnp.zeros((heads, 2 * nq), jnp.float32)
        acc = jnp.zeros((nq, d), jnp.float32)
        if "A" in which:
            q = q_ref[s]
            zero = jnp.zeros_like(q)
            w = jnp.concatenate([jnp.concatenate([q, zero], 1), jnp.concatenate([zero, q], 1)], 0)
        m1 = fold(m8, jnp.maximum, jnp.max)
        for b in range(nblk):
            if "C" in which:
                acc = values(s - 2, b, acc)
            if "B" in which:
                l = weights(b, m1 * c2, l)
            if "A" in which:
                m = scores(s, b, w, m)
        if "C" in which:
            send[pl.ds((s - 2) * per, per)] = acc.reshape(per, SUB, d).astype(send.dtype)
            stat[s - 2] = jnp.where(first, m2, fold(l8, jnp.add, jnp.sum))
        return m, l, m1

    def shape_of(c):
        base, g = chunks[c]
        r = g * per // size
        return base, g, r

    def rows_of(c, o):
        base, _, r = shape_of(c)
        return pl.ds(base * per + o * r, r)

    def seq_of(c, o):
        base, _, r = shape_of(c)
        return base + (o * r) // per

    def remote(src, dst, out, into, j):
        return pltpu.make_async_remote_copy(src, dst, out, into, device_id={"sp": j}, device_id_type=pl.DeviceIdType.MESH)

    def wait_for(ref, sem):
        pltpu.make_async_copy(ref, ref, sem).wait()

    def send_parts(c):
        for i in range(1, size):
            j = lax.rem(me + i, size)
            o = owner(j)
            remote(send.at[rows_of(c, o)], recv[c].at[me], sems.at[PART_OUT, c], sems.at[PART_IN, c], j).start()
            remote(stat.at[seq_of(c, o)], rstat[c].at[me], sems.at[STAT_OUT, c], sems.at[STAT_IN, c], j).start()

    def combine(c, direct):
        base, g, r = shape_of(c)
        o = owner(me)
        recv[c][me] = send[rows_of(c, o)]
        rstat[c][me] = stat[seq_of(c, o)]
        wait_for(rstat[c].at[pl.ds(0, size - 1)], sems.at[STAT_IN, c])
        wait_for(recv[c].at[pl.ds(0, size - 1)], sems.at[PART_IN, c])
        st = rstat[c][...].reshape(size, 2 * nq)
        e = jnp.exp2((st - jnp.max(st, 0, keepdims=True)) * c2)
        f = e / jnp.sum(e * pltpu.roll(st, nq, 1), 0, keepdims=True)
        cols[...] = f.T
        f = cols[pl.ds(pl.multiple_of(lax.rem(o * r, per) * SUB, SUB), r * SUB), :]
        acc = jnp.zeros((r * SUB, d), jnp.float32)
        for j in range(size):
            acc = acc + recv[c][j].astype(jnp.float32).reshape(r * SUB, d) * f[:, j : j + 1]
        mine = rows_of(c, o)
        o_ref[mine] = acc.reshape(r, SUB, d).astype(o_ref.dtype)
        if direct:
            peers = [lax.rem(me + i, size) for i in range(1, size)]
        else:
            peers = [lax.rem(z + i, zs) * CORES + core for i in range(1, zs)]
        for j in peers:
            remote(o_ref.at[mine], o_ref.at[mine], sems.at[RES_OUT, c], sems.at[RES_IN, c], j).start()

    def count(c, k):
        return o_ref.at[pl.ds(0, k * shape_of(c)[2])]

    def pass_on(c):
        base, g, r = shape_of(c)
        wait_for(count(c, zs - 1), sems.at[RES_IN, c])
        own = o_ref.at[pl.ds(base * per + core * zs * r, zs * r)]
        remote(own, own, sems.at[PASS_OUT, c], sems.at[PASS_IN, c], z * CORES + lax.rem(core + 1, CORES)).start()

    last = nc - 1
    ends = [base + g for base, g in chunks]
    events = {}
    for c in range(nc):
        events.setdefault(ends[c], []).append(functools.partial(send_parts, c))
    late = []
    for c in range(last):
        at = ends[c] + chunks[c][1] + chunks[c][1] // 2
        if at < n - 1:
            events.setdefault(at, []).append(functools.partial(combine, c, False))
        else:
            late.append(c)
    early = [c for c in range(last) if c not in late]

    state = (jnp.zeros((heads, 2 * nq), jnp.float32), jnp.zeros((heads, 2 * nq), jnp.float32), jnp.zeros((1, 2 * nq), jnp.float32))

    def refill(copy, s):
        @pl.when(s + SLOTS < n)
        def _():
            copy(s + SLOTS).start()

    kcopy(0).wait()
    state = stage(0, state, "A")
    refill(kcopy, 0)
    kcopy(1).wait()
    state = stage(1, state, "BA")
    refill(kcopy, 1)

    def body(s, state):
        kcopy(s).wait()
        vcopy(s - 2).wait()
        state = stage(s, state, "ABC")
        refill(kcopy, s)
        refill(vcopy, s - 2)
        return state

    at = 2
    waited = False
    for e in sorted(x for x in events if x <= n - 2) + [n - 2]:
        if e + 2 > at:
            state = lax.fori_loop(at, e + 2, body, state)
            at = e + 2
        if not waited:
            pl.semaphore_wait(barrier, size - 1)
            waited = True
        for run in events.pop(e, []):
            run()
    vcopy(n - 2).wait()
    state = stage(n, state, "BC")
    for run in events.pop(n - 1, []):
        run()
    vcopy(n - 1).wait()
    state = stage(n + 1, state, "C")
    for run in events.pop(n, []):
        run()
    for c in early:
        pass_on(c)
    for c in late:
        combine(c, False)
    combine(last, True)
    for c in late:
        pass_on(c)
    for c in range(last):
        base, g, r = shape_of(c)
        wait_for(count(c, zs), sems.at[PASS_IN, c])
    wait_for(count(last, size - 1), sems.at[RES_IN, last])
    for c in range(nc):
        wait_for(recv[c].at[pl.ds(0, size - 1)], sems.at[PART_OUT, c])
        wait_for(rstat[c].at[pl.ds(0, size - 1)], sems.at[STAT_OUT, c])
        wait_for(count(c, size - 1 if c == last else zs - 1), sems.at[RES_OUT, c])
        if c < last:
            wait_for(count(c, zs), sems.at[PASS_OUT, c])


def solution(mesh):
    size = mesh.shape["sp"]

    def step(q, k, v):
        n, nq, d = q.shape
        t, heads = k.shape[1:3]
        per = nq // SUB
        chunks = chunks_of(n, size // per)
        nc = len(chunks)
        rows = t * heads
        out = pl.pallas_call(
            functools.partial(kernel, size, chunks, d**-0.5, heads),
            out_shape=jax.ShapeDtypeStruct((n * per, SUB, d), q.dtype),
            in_specs=[pl.BlockSpec(memory_space=pltpu.VMEM), pl.BlockSpec(memory_space=pl.ANY), pl.BlockSpec(memory_space=pl.ANY)],
            out_specs=pl.BlockSpec(memory_space=pltpu.VMEM),
            scratch_shapes=[
                pltpu.VMEM((SLOTS, rows, d), k.dtype),
                pltpu.VMEM((SLOTS, rows, d), v.dtype),
                pltpu.VMEM((rows // 2, 2 * nq), jnp.float32),
                pltpu.VMEM((2 * nq, rows // 2), jnp.bfloat16),
                pltpu.VMEM((n * per, SUB, d), jnp.bfloat16),
                pltpu.VMEM((n, 1, 2 * nq), jnp.float32),
                pltpu.VMEM((2 * nq, size), jnp.float32),
                *[pltpu.VMEM((size, g * per // size, SUB, d), jnp.bfloat16) for _, g in chunks],
                *[pltpu.VMEM((size, 1, 2 * nq), jnp.float32) for _ in chunks],
                pltpu.SemaphoreType.DMA((SLOTS,)),
                pltpu.SemaphoreType.DMA((SLOTS,)),
                pltpu.SemaphoreType.DMA((8, nc)),
            ],
            compiler_params=pltpu.CompilerParams(collective_id=0, has_side_effects=True, vmem_limit_bytes=60 * 1024 * 1024),
        )(q, k.reshape(n, rows, d), v.reshape(n, rows, d))
        return out.reshape(q.shape)

    return jax.shard_map(
        step,
        mesh=mesh,
        in_specs=(P("dp", None, None), P("dp", "sp", None, None), P("dp", "sp", None, None)),
        out_specs=P("dp", None, None),
        check_vma=False,
    )
```

```python
import functools

import jax
import jax.numpy as jnp
from jax import lax
from jax.experimental import pallas as pl
from jax.experimental.pallas import tpu as pltpu
from jax.sharding import PartitionSpec as P

SLOTS = 8
BLOCK = 512
CORES = 2
SUB = 8
LOG2E = 1.4426950408889634


def chunks_of(n, unit):
    sizes = [4 * unit] * (n // (4 * unit) - 1) + [2 * unit, unit, unit]
    assert sum(sizes) == n
    return [(sum(sizes[:i]), g) for i, g in enumerate(sizes)]


def kernel(size, chunks, scale, heads, q_hbm, k_hbm, v_hbm, o_ref, q_ref, kbuf, vbuf, sb0, sb1, pb0, pb1, send, stat, cols, *rest):
    nc = len(chunks)
    recv, rstat = rest[:nc], rest[nc : 2 * nc]
    qsem, ksem, vsem, sems = rest[2 * nc :]
    sbufs, pbufs = (sb0, sb1), (pb0, pb1)
    PART_OUT, PART_IN, STAT_OUT, STAT_IN, RES_OUT, RES_IN, PASS_OUT, PASS_IN = range(8)
    n, nq, d = q_hbm.shape
    rows = k_hbm.shape[1]
    half = rows // 2
    nblk = half // BLOCK
    per = nq // SUB
    c2 = scale * LOG2E
    me = lax.axis_index("sp")
    zs = size // CORES
    core, z = lax.rem(me, CORES), me // CORES

    def owner(j):
        return lax.rem(j, CORES) * zs + j // CORES

    barrier = pltpu.get_barrier_semaphore()
    for i in range(1, size):
        pl.semaphore_signal(barrier, inc=1, device_id={"sp": lax.rem(me + i, size)}, device_id_type=pl.DeviceIdType.MESH)

    def kcopy(s):
        return pltpu.make_async_copy(k_hbm.at[s], kbuf.at[lax.rem(s, SLOTS)], ksem.at[lax.rem(s, SLOTS)])

    def vcopy(s):
        return pltpu.make_async_copy(v_hbm.at[s], vbuf.at[lax.rem(s, SLOTS)], vsem.at[lax.rem(s, SLOTS)])

    qcopy = pltpu.make_async_copy(q_hbm, q_ref, qsem)
    qcopy.start()
    for s in range(SLOTS):
        kcopy(s).start()
        vcopy(s).start()

    row = lax.broadcasted_iota(jnp.int32, (heads, 2 * nq), 0)
    lane = lax.broadcasted_iota(jnp.int32, (heads, 2 * nq), 1)
    keep = row == lax.rem(lane, nq) // (nq // heads)
    first = lax.broadcasted_iota(jnp.int32, (1, 2 * nq), 1) < nq

    def scores(s, b, w, m, sbuf):
        slot = lax.rem(s, SLOTS)
        k0 = kbuf[slot, pl.ds(b * BLOCK, BLOCK), :]
        k1 = kbuf[slot, pl.ds(half + b * BLOCK, BLOCK), :]
        x = lax.dot_general(jnp.concatenate([k0, k1], 1), w, (((1,), (1,)), ((), ())), preferred_element_type=jnp.float32)
        x = jnp.where(keep[None], x.reshape(BLOCK // heads, heads, 2 * nq), -jnp.inf)
        sbuf[pl.ds(b * BLOCK, BLOCK), :] = x.reshape(BLOCK, 2 * nq)
        return jnp.maximum(m, jnp.max(x, 0))

    def weights(b, mc, l, sbuf, pbuf):
        p = jnp.exp2(sbuf[pl.ds(b * BLOCK, BLOCK), :] * c2 - mc)
        pbuf[:, pl.ds(b * BLOCK, BLOCK)] = p.astype(jnp.bfloat16).T
        return l + jnp.sum(p.reshape(BLOCK // heads, heads, 2 * nq), 0)

    def values(s, b, acc, pbuf):
        slot = lax.rem(s, SLOTS)
        at = pl.ds(b * BLOCK, BLOCK)
        acc = acc + jnp.dot(pbuf[:nq, at], vbuf[slot, at, :], preferred_element_type=jnp.float32)
        return acc + jnp.dot(pbuf[nq:, at], vbuf[slot, pl.ds(half + b * BLOCK, BLOCK), :], preferred_element_type=jnp.float32)

    def fold(x, op, reduce):
        x = reduce(x, 0, keepdims=True)
        return op(x, pltpu.roll(x, nq, 1))

    def stat_of(m, l):
        return jnp.where(first, m, fold(l, jnp.add, jnp.sum))

    def stage(s, side, state, which):
        m8, l8, m2 = state
        m = jnp.full((heads, 2 * nq), -jnp.inf, jnp.float32)
        l = jnp.zeros((heads, 2 * nq), jnp.float32)
        acc = jnp.zeros((nq, d), jnp.float32)
        if "A" in which:
            q = q_ref[s]
            zero = jnp.zeros_like(q)
            w = jnp.concatenate([jnp.concatenate([q, zero], 1), jnp.concatenate([zero, q], 1)], 0)
        m1 = fold(m8, jnp.maximum, jnp.max)
        for b in range(nblk):
            if "C" in which:
                acc = values(s - 2, b, acc, pbufs[side])
            if "B" in which:
                l = weights(b, m1 * c2, l, sbufs[1 - side], pbufs[1 - side])
            if "A" in which:
                m = scores(s, b, w, m, sbufs[side])
        if "C" in which:
            send[pl.ds((s - 2) * per, per)] = acc.reshape(per, SUB, d).astype(send.dtype)
            if "B" in which:
                stat[s - 2] = stat_of(m2, l8)
        return m, l, m1

    def shape_of(c):
        base, g = chunks[c]
        r = g * per // size
        return base, g, r

    def rows_of(c, o):
        base, _, r = shape_of(c)
        return pl.ds(base * per + o * r, r)

    def seq_of(c, o):
        base, _, r = shape_of(c)
        return base + (o * r) // per

    def remote(src, dst, out, into, j):
        return pltpu.make_async_remote_copy(src, dst, out, into, device_id={"sp": j}, device_id_type=pl.DeviceIdType.MESH)

    def wait_for(ref, sem):
        pltpu.make_async_copy(ref, ref, sem).wait()

    def peers():
        for i in [x for k in range(zs // 2) for x in (zs // 2 - k, zs // 2 + k)[: 1 + (k > 0)]]:
            for k in range(CORES):
                yield lax.rem(z + i, zs) * CORES + lax.rem(core + k, CORES)
        for k in range(1, CORES):
            yield z * CORES + lax.rem(core + k, CORES)

    def send_part(c, j):
        remote(send.at[rows_of(c, owner(j))], recv[c].at[me], sems.at[PART_OUT, c], sems.at[PART_IN, c], j).start()

    def send_stat(c, j):
        remote(stat.at[seq_of(c, owner(j))], rstat[c].at[me], sems.at[STAT_OUT, c], sems.at[STAT_IN, c], j).start()

    def send_parts(c):
        for j in peers():
            send_part(c, j)
            send_stat(c, j)

    def combine(c, direct):
        base, g, r = shape_of(c)
        o = owner(me)
        recv[c][me] = send[rows_of(c, o)]
        rstat[c][me] = stat[seq_of(c, o)]
        wait_for(rstat[c].at[pl.ds(0, size - 1)], sems.at[STAT_IN, c])
        wait_for(recv[c].at[pl.ds(0, size - 1)], sems.at[PART_IN, c])
        st = rstat[c][...].reshape(size, 2 * nq)
        e = jnp.exp2((st - jnp.max(st, 0, keepdims=True)) * c2)
        f = e / jnp.sum(e * pltpu.roll(st, nq, 1), 0, keepdims=True)
        cols[...] = f.T
        f = cols[pl.ds(pl.multiple_of(lax.rem(o * r, per) * SUB, SUB), r * SUB), :]
        acc = jnp.zeros((r * SUB, d), jnp.float32)
        for j in range(size):
            acc = acc + recv[c][j].astype(jnp.float32).reshape(r * SUB, d) * f[:, j : j + 1]
        mine = rows_of(c, o)
        o_ref[mine] = acc.reshape(r, SUB, d).astype(o_ref.dtype)
        for i, j in enumerate(peers()):
            if direct or i % CORES == 0 and i < (zs - 1) * CORES:
                remote(o_ref.at[mine], o_ref.at[mine], sems.at[RES_OUT, c], sems.at[RES_IN, c], j).start()

    def count(c, k):
        return o_ref.at[pl.ds(0, k * shape_of(c)[2])]

    def pass_on(c):
        base, g, r = shape_of(c)
        wait_for(count(c, zs - 1), sems.at[RES_IN, c])
        own = o_ref.at[pl.ds(base * per + core * zs * r, zs * r)]
        remote(own, own, sems.at[PASS_OUT, c], sems.at[PASS_IN, c], z * CORES + lax.rem(core + 1, CORES)).start()

    last = nc - 1
    ends = [base + g for base, g in chunks]
    events = {}
    for c in range(last):
        events.setdefault(ends[c], []).append(functools.partial(send_parts, c))
    late = []
    for c in range(last):
        at = ends[c] + chunks[c][1] + chunks[c][1] // 2
        if at < n - 1:
            events.setdefault(at, []).append(functools.partial(combine, c, False))
        else:
            late.append(c)
    early = [c for c in range(last) if c not in late]

    state = (jnp.zeros((heads, 2 * nq), jnp.float32), jnp.zeros((heads, 2 * nq), jnp.float32), jnp.zeros((1, 2 * nq), jnp.float32))

    def refill(copy, s):
        @pl.when(s + SLOTS < n)
        def _():
            copy(s + SLOTS).start()

    qcopy.wait()
    kcopy(0).wait()
    state = stage(0, 0, state, "A")
    refill(kcopy, 0)
    kcopy(1).wait()
    state = stage(1, 1, state, "BA")
    refill(kcopy, 1)

    def body(i, state):
        s = 2 * i
        for u in range(2):
            kcopy(s + u).wait()
            vcopy(s + u - 2).wait()
        for u in range(2):
            state = stage(s + u, u, state, "ABC")
        for u in range(2):
            refill(kcopy, s + u)
            refill(vcopy, s + u - 2)
        return state

    at = 2
    waited = False
    for e in sorted(x for x in events if x <= n - 2):
        state = lax.fori_loop(at // 2, e // 2 + 1, body, state)
        at = e + 2
        if not waited:
            pl.semaphore_wait(barrier, size - 1)
            waited = True
        for run in events.pop(e):
            run()
    assert at == n
    vcopy(n - 2).wait()
    m8, l8, m2 = stage(n, 0, state, "BC")
    stat[n - 1] = stat_of(m2, l8)
    for j in peers():
        send_stat(last, j)
    for i in range(zs):
        if i:
            send_part(last, lax.rem(z + i, zs) * CORES)
    @pl.when(core != 0)
    def _():
        send_part(last, z * CORES)
    vcopy(n - 1).wait()
    stage(n + 1, 1, (m8, l8, m2), "C")
    for i in range(zs):
        if i:
            send_part(last, lax.rem(z + i, zs) * CORES + 1)
    @pl.when(core == 0)
    def _():
        send_part(last, z * CORES + 1)
    for c in early:
        pass_on(c)
    for c in late:
        combine(c, False)
    combine(last, True)
    for c in late:
        pass_on(c)
    for c in range(last):
        base, g, r = shape_of(c)
        wait_for(count(c, zs), sems.at[PASS_IN, c])
    wait_for(count(last, size - 1), sems.at[RES_IN, last])
    for c in range(nc):
        wait_for(recv[c].at[pl.ds(0, size - 1)], sems.at[PART_OUT, c])
        wait_for(rstat[c].at[pl.ds(0, size - 1)], sems.at[STAT_OUT, c])
        wait_for(count(c, size - 1 if c == last else zs - 1), sems.at[RES_OUT, c])
        if c < last:
            wait_for(count(c, zs), sems.at[PASS_OUT, c])


def solution(mesh):
    size = mesh.shape["sp"]

    def step(q, k, v):
        n, nq, d = q.shape
        t, heads = k.shape[1:3]
        per = nq // SUB
        chunks = chunks_of(n, size // per)
        nc = len(chunks)
        rows = t * heads
        out = pl.pallas_call(
            functools.partial(kernel, size, chunks, d**-0.5, heads),
            out_shape=pltpu.VMEM((n * per, SUB, d), q.dtype),
            in_specs=[pl.BlockSpec(memory_space=pl.ANY)] * 3,
            out_specs=pl.BlockSpec(memory_space=pltpu.VMEM),
            scratch_shapes=[
                pltpu.VMEM(q.shape, q.dtype),
                pltpu.VMEM((SLOTS, rows, d), k.dtype),
                pltpu.VMEM((SLOTS, rows, d), v.dtype),
                *[pltpu.VMEM((rows // 2, 2 * nq), jnp.float32)] * 2,
                *[pltpu.VMEM((2 * nq, rows // 2), jnp.bfloat16)] * 2,
                pltpu.VMEM((n * per, SUB, d), jnp.bfloat16),
                pltpu.VMEM((n, 1, 2 * nq), jnp.float32),
                pltpu.VMEM((2 * nq, size), jnp.float32),
                *[pltpu.VMEM((size, g * per // size, SUB, d), jnp.bfloat16) for _, g in chunks],
                *[pltpu.VMEM((size, 1, 2 * nq), jnp.float32) for _ in chunks],
                pltpu.SemaphoreType.DMA,
                pltpu.SemaphoreType.DMA((SLOTS,)),
                pltpu.SemaphoreType.DMA((SLOTS,)),
                pltpu.SemaphoreType.DMA((8, nc)),
            ],
            compiler_params=pltpu.CompilerParams(collective_id=0, has_side_effects=True, vmem_limit_bytes=60 * 1024 * 1024),
        )(q, k.reshape(n, rows, d), v.reshape(n, rows, d))
        return out.reshape(q.shape)

    return jax.shard_map(
        step,
        mesh=mesh,
        in_specs=(P("dp", None, None), P("dp", "sp", None, None), P("dp", "sp", None, None)),
        out_specs=P("dp", None, None),
        check_vma=False,
    )
```

```python
import functools

import jax
import jax.numpy as jnp
from jax import lax
from jax.experimental import pallas as pl
from jax.experimental.pallas import tpu as pltpu
from jax.sharding import PartitionSpec as P

SLOTS = 8
BLOCK = 512
CORES = 2
JOIN_LAG = 10
SUB = 8
LOG2E = 1.4426950408889634


def chunks_of(n, unit):
    sizes = [8 * unit, 4 * unit, 2 * unit, 2 * unit]
    assert sum(sizes) == n
    return [(sum(sizes[:i]), g) for i, g in enumerate(sizes)]


def kernel(size, chunks, scale, heads, q_hbm, k_hbm, v_hbm, o_ref, q_ref, kbuf, vbuf, sb0, sb1, pb0, pb1, send, stat, cols, *rest):
    nc = len(chunks)
    recv, rstat = rest[:nc], rest[nc : 2 * nc]
    qsem, ksem, vsem, sems = rest[2 * nc :]
    sbufs, pbufs = (sb0, sb1), (pb0, pb1)
    PART_OUT, PART_IN, STAT_OUT, STAT_IN, RES_OUT, RES_IN, PASS_OUT, PASS_IN = range(8)
    n, nq, d = q_hbm.shape
    rows = k_hbm.shape[1]
    half = rows // 2
    nblk = half // BLOCK
    per = nq // SUB
    c2 = scale * LOG2E
    me = lax.axis_index("sp")
    zs = size // CORES
    core, z = lax.rem(me, CORES), me // CORES

    def spread(z):
        return lax.rem(z * (zs // 2 + 1), zs)

    def owner(j):
        return lax.rem(j, CORES) * zs + spread(j // CORES)

    def device(o):
        return spread(lax.rem(o, zs)) * CORES + o // zs

    barrier = pltpu.get_barrier_semaphore()
    for i in range(1, size):
        pl.semaphore_signal(barrier, inc=1, device_id={"sp": lax.rem(me + i, size)}, device_id_type=pl.DeviceIdType.MESH)

    def kcopy(s):
        return pltpu.make_async_copy(k_hbm.at[s], kbuf.at[lax.rem(s, SLOTS)], ksem.at[lax.rem(s, SLOTS)])

    def vcopy(s):
        return pltpu.make_async_copy(v_hbm.at[s], vbuf.at[lax.rem(s, SLOTS)], vsem.at[lax.rem(s, SLOTS)])

    qcopy = pltpu.make_async_copy(q_hbm, q_ref, qsem)
    qcopy.start()
    for s in range(SLOTS):
        kcopy(s).start()
        vcopy(s).start()

    row = lax.broadcasted_iota(jnp.int32, (heads, 2 * nq), 0)
    lane = lax.broadcasted_iota(jnp.int32, (heads, 2 * nq), 1)
    keep = row == lax.rem(lane, nq) // (nq // heads)
    first = lax.broadcasted_iota(jnp.int32, (1, 2 * nq), 1) < nq

    def scores(s, b, w, m, sbuf):
        slot = lax.rem(s, SLOTS)
        k0 = kbuf[slot, pl.ds(b * BLOCK, BLOCK), :]
        k1 = kbuf[slot, pl.ds(half + b * BLOCK, BLOCK), :]
        x = lax.dot_general(jnp.concatenate([k0, k1], 1), w, (((1,), (1,)), ((), ())), preferred_element_type=jnp.float32)
        x = jnp.where(keep[None], x.reshape(BLOCK // heads, heads, 2 * nq), -jnp.inf)
        sbuf[pl.ds(b * BLOCK, BLOCK), :] = x.reshape(BLOCK, 2 * nq)
        return jnp.maximum(m, jnp.max(x, 0))

    def weights(b, mc, l, sbuf, pbuf):
        p = jnp.exp2(sbuf[pl.ds(b * BLOCK, BLOCK), :] * c2 - mc)
        pbuf[:, pl.ds(b * BLOCK, BLOCK)] = p.astype(jnp.bfloat16).T
        return l + jnp.sum(p.reshape(BLOCK // heads, heads, 2 * nq), 0)

    def values(s, b, acc, pbuf):
        slot = lax.rem(s, SLOTS)
        at = pl.ds(b * BLOCK, BLOCK)
        acc = acc + jnp.dot(pbuf[:nq, at], vbuf[slot, at, :], preferred_element_type=jnp.float32)
        return acc + jnp.dot(pbuf[nq:, at], vbuf[slot, pl.ds(half + b * BLOCK, BLOCK), :], preferred_element_type=jnp.float32)

    def fold(x, op, reduce):
        x = reduce(x, 0, keepdims=True)
        return op(x, pltpu.roll(x, nq, 1))

    def stat_of(m, l):
        return jnp.where(first, m, fold(l, jnp.add, jnp.sum))

    def stage(s, side, state, which):
        m8, l8, m2 = state
        m = jnp.full((heads, 2 * nq), -jnp.inf, jnp.float32)
        l = jnp.zeros((heads, 2 * nq), jnp.float32)
        acc = jnp.zeros((nq, d), jnp.float32)
        if "A" in which:
            q = q_ref[s]
            zero = jnp.zeros_like(q)
            w = jnp.concatenate([jnp.concatenate([q, zero], 1), jnp.concatenate([zero, q], 1)], 0)
        m1 = fold(m8, jnp.maximum, jnp.max)
        for b in range(nblk):
            if "C" in which:
                acc = values(s - 2, b, acc, pbufs[side])
            if "B" in which:
                l = weights(b, m1 * c2, l, sbufs[1 - side], pbufs[1 - side])
            if "A" in which:
                m = scores(s, b, w, m, sbufs[side])
        if "C" in which:
            send[pl.ds((s - 2) * per, per)] = acc.reshape(per, SUB, d).astype(send.dtype)
            if "B" in which:
                stat[s - 2] = stat_of(m2, l8)
        return m, l, m1

    def shape_of(c):
        base, g = chunks[c]
        r = g * per // size
        return base, g, r

    def rows_of(c, o):
        base, _, r = shape_of(c)
        return pl.ds(base * per + o * r, r)

    def seq_of(c, o):
        base, _, r = shape_of(c)
        return base + (o * r) // per

    def remote(src, dst, out, into, j):
        return pltpu.make_async_remote_copy(src, dst, out, into, device_id={"sp": j}, device_id_type=pl.DeviceIdType.MESH)

    def wait_for(ref, sem):
        pltpu.make_async_copy(ref, ref, sem).wait()

    def peers():
        for i in [x for k in range(zs // 2) for x in (zs // 2 - k, zs // 2 + k)[: 1 + (k > 0)]]:
            for k in range(CORES):
                yield lax.rem(z + i, zs) * CORES + lax.rem(core + k, CORES)
        for k in range(1, CORES):
            yield z * CORES + lax.rem(core + k, CORES)

    def owners_of(c, s):
        base, _, r = shape_of(c)
        return [(s - base) * (per // r) + i for i in range(per // r)]

    def to_owners(c, s, part=True, stats=True):
        for o in owners_of(c, s):
            j = device(o)

            @pl.when(j != me)
            def _():
                if stats:
                    remote(stat.at[s], rstat[c].at[me], sems.at[STAT_OUT, c], sems.at[STAT_IN, c], j).start()
                if part:
                    remote(send.at[rows_of(c, o)], recv[c].at[me], sems.at[PART_OUT, c], sems.at[PART_IN, c], j).start()

    def combine(c, direct):
        base, g, r = shape_of(c)
        o = owner(me)
        recv[c][me] = send[rows_of(c, o)]
        rstat[c][me] = stat[seq_of(c, o)]
        wait_for(rstat[c].at[pl.ds(0, size - 1)], sems.at[STAT_IN, c])
        wait_for(recv[c].at[pl.ds(0, size - 1)], sems.at[PART_IN, c])
        st = rstat[c][...].reshape(size, 2 * nq)
        e = jnp.exp2((st - jnp.max(st, 0, keepdims=True)) * c2)
        f = e / jnp.sum(e * pltpu.roll(st, nq, 1), 0, keepdims=True)
        cols[...] = f.T
        f = cols[pl.ds(pl.multiple_of(lax.rem(o * r, per) * SUB, SUB), r * SUB), :]
        acc = jnp.zeros((r * SUB, d), jnp.float32)
        for j in range(size):
            acc = acc + recv[c][j].astype(jnp.float32).reshape(r * SUB, d) * f[:, j : j + 1]
        mine = rows_of(c, o)
        o_ref[mine] = acc.reshape(r, SUB, d).astype(o_ref.dtype)
        for i, j in enumerate(peers()):
            if direct or i % CORES == 0 and i < (zs - 1) * CORES:
                remote(o_ref.at[mine], o_ref.at[mine], sems.at[RES_OUT, c], sems.at[RES_IN, c], j).start()

    def count(c, k):
        return o_ref.at[pl.ds(0, k * shape_of(c)[2])]

    def pass_on(c):
        base, g, r = shape_of(c)
        wait_for(count(c, zs - 1), sems.at[RES_IN, c])
        own = o_ref.at[pl.ds(base * per + core * zs * r, zs * r)]
        remote(own, own, sems.at[PASS_OUT, c], sems.at[PASS_IN, c], z * CORES + lax.rem(core + 1, CORES)).start()

    last = nc - 1
    joined = JOIN_LAG + chunks[0][1]

    state = (jnp.zeros((heads, 2 * nq), jnp.float32), jnp.zeros((heads, 2 * nq), jnp.float32), jnp.zeros((1, 2 * nq), jnp.float32))

    def refill(copy, s):
        @pl.when(s + SLOTS < n)
        def _():
            copy(s + SLOTS).start()

    qcopy.wait()
    kcopy(0).wait()
    state = stage(0, 0, state, "A")
    refill(kcopy, 0)
    kcopy(1).wait()
    state = stage(1, 1, state, "BA")
    refill(kcopy, 1)

    def body(c, i, state):
        s = 2 * i
        for u in range(2):
            kcopy(s + u).wait()
            vcopy(s + u - 2).wait()
        for u in range(2):
            state = stage(s + u, u, state, "ABC")
        for u in range(2):
            refill(kcopy, s + u)
            refill(vcopy, s + u - 2)
        for u in range(2):
            to_owners(c, s + u - 2)
        return state

    pl.semaphore_wait(barrier, size - 1)
    for c, (base, g) in enumerate(chunks):
        for lo, hi in ((base, min(base + g, joined)), (max(base, joined), min(base + g, n - 2))):
            if lo < hi:
                state = lax.fori_loop(lo // 2 + 1, hi // 2 + 1, functools.partial(body, c), state)
                if hi == joined:
                    combine(0, False)
    vcopy(n - 2).wait()
    m8, l8, m2 = stage(n, 0, state, "BC")
    stat[n - 1] = stat_of(m2, l8)
    to_owners(last, n - 2)
    to_owners(last, n - 1, part=False)
    vcopy(n - 1).wait()
    stage(n + 1, 1, (m8, l8, m2), "C")
    to_owners(last, n - 1, stats=False)
    for c in range(1, last):
        combine(c, False)
    pass_on(0)
    combine(last, True)
    for c in range(1, last):
        pass_on(c)
    for c in range(last):
        base, g, r = shape_of(c)
        wait_for(count(c, zs), sems.at[PASS_IN, c])
    wait_for(count(last, size - 1), sems.at[RES_IN, last])
    for c in range(nc):
        wait_for(recv[c].at[pl.ds(0, size - 1)], sems.at[PART_OUT, c])
        wait_for(rstat[c].at[pl.ds(0, size - 1)], sems.at[STAT_OUT, c])
        wait_for(count(c, size - 1 if c == last else zs - 1), sems.at[RES_OUT, c])
        if c < last:
            wait_for(count(c, zs), sems.at[PASS_OUT, c])


def solution(mesh):
    size = mesh.shape["sp"]

    def step(q, k, v):
        n, nq, d = q.shape
        t, heads = k.shape[1:3]
        per = nq // SUB
        chunks = chunks_of(n, size // per)
        nc = len(chunks)
        rows = t * heads
        out = pl.pallas_call(
            functools.partial(kernel, size, chunks, d**-0.5, heads),
            out_shape=pltpu.VMEM((n * per, SUB, d), q.dtype),
            in_specs=[pl.BlockSpec(memory_space=pl.ANY)] * 3,
            out_specs=pl.BlockSpec(memory_space=pltpu.VMEM),
            scratch_shapes=[
                pltpu.VMEM(q.shape, q.dtype),
                pltpu.VMEM((SLOTS, rows, d), k.dtype),
                pltpu.VMEM((SLOTS, rows, d), v.dtype),
                *[pltpu.VMEM((rows // 2, 2 * nq), jnp.float32)] * 2,
                *[pltpu.VMEM((2 * nq, rows // 2), jnp.bfloat16)] * 2,
                pltpu.VMEM((n * per, SUB, d), jnp.bfloat16),
                pltpu.VMEM((n, 1, 2 * nq), jnp.float32),
                pltpu.VMEM((2 * nq, size), jnp.float32),
                *[pltpu.VMEM((size, g * per // size, SUB, d), jnp.bfloat16) for _, g in chunks],
                *[pltpu.VMEM((size, 1, 2 * nq), jnp.float32) for _ in chunks],
                pltpu.SemaphoreType.DMA,
                pltpu.SemaphoreType.DMA((SLOTS,)),
                pltpu.SemaphoreType.DMA((SLOTS,)),
                pltpu.SemaphoreType.DMA((8, nc)),
            ],
            compiler_params=pltpu.CompilerParams(collective_id=0, has_side_effects=True, vmem_limit_bytes=60 * 1024 * 1024),
        )(q, k.reshape(n, rows, d), v.reshape(n, rows, d))
        return out.reshape(q.shape)

    return jax.shard_map(
        step,
        mesh=mesh,
        in_specs=(P("dp", None, None), P("dp", "sp", None, None), P("dp", "sp", None, None)),
        out_specs=P("dp", None, None),
        check_vma=False,
    )
```

```python
import functools

import jax
import jax.numpy as jnp
from jax import lax
from jax.experimental import pallas as pl
from jax.experimental.pallas import tpu as pltpu
from jax.sharding import PartitionSpec as P

SLOTS = 8
BLOCK = 512
CORES = 2
JOIN_LAG = 10
SUB = 8
LOG2E = 1.4426950408889634


def chunks_of(n, unit):
    sizes = [8 * unit, 4 * unit, 2 * unit, 2 * unit]
    assert sum(sizes) == n
    return [(sum(sizes[:i]), g) for i, g in enumerate(sizes)]


def kernel(size, chunks, scale, heads, q_hbm, k_hbm, v_hbm, o_ref, q_ref, kbuf, vbuf, sb0, sb1, pb0, pb1, send, stat, cols, *rest):
    nc = len(chunks)
    recv, rstat = rest[:nc], rest[nc : 2 * nc]
    qsem, ksem, vsem, sems = rest[2 * nc :]
    sbufs, pbufs = (sb0, sb1), (pb0, pb1)
    PART_OUT, PART_IN, STAT_OUT, STAT_IN, RES_OUT, RES_IN, PASS_OUT, PASS_IN = range(8)
    n, nq, d = q_hbm.shape
    rows = k_hbm.shape[1]
    half = rows // 2
    nblk = half // BLOCK
    per = nq // SUB
    c2 = scale * LOG2E
    me = lax.axis_index("sp")
    zs = size // CORES
    core, z = lax.rem(me, CORES), me // CORES

    def spread(z):
        return lax.rem(z * (zs // 2 + 1), zs)

    def owner(j):
        return lax.rem(j, CORES) * zs + spread(j // CORES)

    def device(o):
        return spread(lax.rem(o, zs)) * CORES + o // zs

    barrier = pltpu.get_barrier_semaphore()
    for i in range(1, size):
        pl.semaphore_signal(barrier, inc=1, device_id={"sp": lax.rem(me + i, size)}, device_id_type=pl.DeviceIdType.MESH)

    def kcopy(s):
        return pltpu.make_async_copy(k_hbm.at[s], kbuf.at[lax.rem(s, SLOTS)], ksem.at[lax.rem(s, SLOTS)])

    def vcopy(s):
        return pltpu.make_async_copy(v_hbm.at[s], vbuf.at[lax.rem(s, SLOTS)], vsem.at[lax.rem(s, SLOTS)])

    qcopy = pltpu.make_async_copy(q_hbm, q_ref, qsem)
    qcopy.start()
    for s in range(SLOTS):
        kcopy(s).start()
        vcopy(s).start()

    row = lax.broadcasted_iota(jnp.int32, (heads, 2 * nq), 0)
    lane = lax.broadcasted_iota(jnp.int32, (heads, 2 * nq), 1)
    keep = row == lax.rem(lane, nq) // (nq // heads)
    first = lax.broadcasted_iota(jnp.int32, (1, 2 * nq), 1) < nq

    def scores(s, b, w, m, sbuf):
        slot = lax.rem(s, SLOTS)
        k0 = kbuf[slot, pl.ds(b * BLOCK, BLOCK), :]
        k1 = kbuf[slot, pl.ds(half + b * BLOCK, BLOCK), :]
        x = lax.dot_general(jnp.concatenate([k0, k1], 1), w, (((1,), (1,)), ((), ())), preferred_element_type=jnp.float32)
        x = jnp.where(keep[None], x.reshape(BLOCK // heads, heads, 2 * nq), -jnp.inf)
        sbuf[pl.ds(b * BLOCK, BLOCK), :] = x.reshape(BLOCK, 2 * nq)
        return jnp.maximum(m, jnp.max(x, 0))

    def weights(b, mc, l, sbuf, pbuf):
        p = jnp.exp2(sbuf[pl.ds(b * BLOCK, BLOCK), :] * c2 - mc)
        pbuf[:, pl.ds(b * BLOCK, BLOCK)] = p.astype(jnp.bfloat16).T
        return l + jnp.sum(p.reshape(BLOCK // heads, heads, 2 * nq), 0)

    def values(s, b, acc, pbuf):
        slot = lax.rem(s, SLOTS)
        at = pl.ds(b * BLOCK, BLOCK)
        acc = acc + jnp.dot(pbuf[:nq, at], vbuf[slot, at, :], preferred_element_type=jnp.float32)
        return acc + jnp.dot(pbuf[nq:, at], vbuf[slot, pl.ds(half + b * BLOCK, BLOCK), :], preferred_element_type=jnp.float32)

    def fold(x, op, reduce):
        x = reduce(x, 0, keepdims=True)
        return op(x, pltpu.roll(x, nq, 1))

    def stat_of(m, l):
        return jnp.where(first, m, fold(l, jnp.add, jnp.sum))

    def stage(s, side, state, which):
        m8, l8, m2 = state
        m = jnp.full((heads, 2 * nq), -jnp.inf, jnp.float32)
        l = jnp.zeros((heads, 2 * nq), jnp.float32)
        acc = jnp.zeros((nq, d), jnp.float32)
        if "A" in which:
            q = q_ref[s]
            zero = jnp.zeros_like(q)
            w = jnp.concatenate([jnp.concatenate([q, zero], 1), jnp.concatenate([zero, q], 1)], 0)
        m1 = fold(m8, jnp.maximum, jnp.max)
        for b in range(nblk):
            if "C" in which:
                acc = values(s - 2, b, acc, pbufs[side])
            if "B" in which:
                l = weights(b, m1 * c2, l, sbufs[1 - side], pbufs[1 - side])
            if "A" in which:
                m = scores(s, b, w, m, sbufs[side])
        if "C" in which:
            send[pl.ds((s - 2) * per, per)] = acc.reshape(per, SUB, d).astype(send.dtype)
            if "B" in which:
                stat[s - 2] = stat_of(m2, l8)
        return m, l, m1

    def shape_of(c):
        base, g = chunks[c]
        r = g * per // size
        return base, g, r

    def rows_of(c, o):
        base, _, r = shape_of(c)
        return pl.ds(base * per + o * r, r)

    def seq_of(c, o):
        base, _, r = shape_of(c)
        return base + (o * r) // per

    def remote(src, dst, out, into, j):
        return pltpu.make_async_remote_copy(src, dst, out, into, device_id={"sp": j}, device_id_type=pl.DeviceIdType.MESH)

    def wait_for(ref, sem):
        pltpu.make_async_copy(ref, ref, sem).wait()

    def peers():
        for i in [x for k in range(zs // 2) for x in (zs // 2 - k, zs // 2 + k)[: 1 + (k > 0)]]:
            for k in range(CORES):
                yield lax.rem(z + i, zs) * CORES + lax.rem(core + k, CORES)
        for k in range(1, CORES):
            yield z * CORES + lax.rem(core + k, CORES)

    def owners_of(c, s):
        base, _, r = shape_of(c)
        return [(s - base) * (per // r) + i for i in range(per // r)]

    def to_owners(c, s, part=True, stats=True):
        for o in owners_of(c, s):
            j = device(o)

            @pl.when(j != me)
            def _():
                if stats:
                    remote(stat.at[s], rstat[c].at[me], sems.at[STAT_OUT, c], sems.at[STAT_IN, c], j).start()
                if part:
                    remote(send.at[rows_of(c, o)], recv[c].at[me], sems.at[PART_OUT, c], sems.at[PART_IN, c], j).start()

    def combine(c, direct):
        base, g, r = shape_of(c)
        o = owner(me)
        rstat[c][me] = stat[seq_of(c, o)]
        wait_for(rstat[c].at[pl.ds(0, size - 1)], sems.at[STAT_IN, c])
        st = rstat[c][...].reshape(size, 2 * nq)
        e = jnp.exp2((st - jnp.max(st, 0, keepdims=True)) * c2)
        f = e / jnp.sum(e * pltpu.roll(st, nq, 1), 0, keepdims=True)
        cols[...] = f.T
        f = cols[pl.ds(pl.multiple_of(lax.rem(o * r, per) * SUB, SUB), r * SUB), :]
        recv[c][me] = send[rows_of(c, o)]
        wait_for(recv[c].at[pl.ds(0, size - 1)], sems.at[PART_IN, c])
        acc = jnp.zeros((r * SUB, d), jnp.float32)
        for j in range(size):
            acc = acc + recv[c][j].astype(jnp.float32).reshape(r * SUB, d) * f[:, j : j + 1]
        mine = rows_of(c, o)
        o_ref[mine] = acc.reshape(r, SUB, d).astype(o_ref.dtype)
        for i, j in enumerate(peers()):
            if direct or i % CORES == 0 and i < (zs - 1) * CORES:
                remote(o_ref.at[mine], o_ref.at[mine], sems.at[RES_OUT, c], sems.at[RES_IN, c], j).start()

    def count(c, k):
        return o_ref.at[pl.ds(0, k * shape_of(c)[2])]

    def pass_on(c):
        base, g, r = shape_of(c)
        wait_for(count(c, zs - 1), sems.at[RES_IN, c])
        own = o_ref.at[pl.ds(base * per + core * zs * r, zs * r)]
        remote(own, own, sems.at[PASS_OUT, c], sems.at[PASS_IN, c], z * CORES + lax.rem(core + 1, CORES)).start()

    last = nc - 1
    assert chunks[0][1] == size and size + JOIN_LAG <= n - 4

    state = (jnp.zeros((heads, 2 * nq), jnp.float32), jnp.zeros((heads, 2 * nq), jnp.float32), jnp.zeros((1, 2 * nq), jnp.float32))

    def refill(copy, s):
        @pl.when(s + SLOTS < n)
        def _():
            copy(s + SLOTS).start()

    qcopy.wait()
    kcopy(0).wait()
    state = stage(0, 0, state, "A")
    refill(kcopy, 0)
    kcopy(1).wait()
    state = stage(1, 1, state, "BA")
    refill(kcopy, 1)

    def body(c, i, state):
        s = 2 * i
        for u in range(2):
            kcopy(s + u).wait()
            vcopy(s + u - 2).wait()
        for u in range(2):
            state = stage(s + u, u, state, "ABC")
        for u in range(2):
            refill(kcopy, s + u)
            refill(vcopy, s + u - 2)
        for u in range(2):
            to_owners(c, s + u - 2)

        @pl.when(owner(me) // 2 == i - 1 - JOIN_LAG // 2)
        def _():
            combine(0, False)

        return state

    pl.semaphore_wait(barrier, size - 1)
    for c, (base, g) in enumerate(chunks):
        lo, hi = base, min(base + g, n - 4)
        if lo < hi:
            state = lax.fori_loop(lo // 2 + 1, hi // 2 + 1, functools.partial(body, c), state)
    for s in (n - 2, n - 1):
        kcopy(s).wait()
        vcopy(s - 2).wait()
        state = stage(s, s % 2, state, "ABC")
        to_owners(last, s - 2)
    vcopy(n - 2).wait()
    m8, l8, m2 = stage(n, 0, state, "BC")
    stat[n - 1] = stat_of(m2, l8)
    to_owners(last, n - 2)
    to_owners(last, n - 1, part=False)
    vcopy(n - 1).wait()
    stage(n + 1, 1, (m8, l8, m2), "C")
    to_owners(last, n - 1, stats=False)
    for c in range(1, last):
        combine(c, False)
    pass_on(0)
    combine(last, True)
    for c in range(1, last):
        pass_on(c)
    for c in range(last):
        base, g, r = shape_of(c)
        wait_for(count(c, zs), sems.at[PASS_IN, c])
    wait_for(count(last, size - 1), sems.at[RES_IN, last])
    for c in range(nc):
        wait_for(recv[c].at[pl.ds(0, size - 1)], sems.at[PART_OUT, c])
        wait_for(rstat[c].at[pl.ds(0, size - 1)], sems.at[STAT_OUT, c])
        wait_for(count(c, size - 1 if c == last else zs - 1), sems.at[RES_OUT, c])
        if c < last:
            wait_for(count(c, zs), sems.at[PASS_OUT, c])


def solution(mesh):
    size = mesh.shape["sp"]

    def step(q, k, v):
        n, nq, d = q.shape
        t, heads = k.shape[1:3]
        per = nq // SUB
        chunks = chunks_of(n, size // per)
        nc = len(chunks)
        rows = t * heads
        out = pl.pallas_call(
            functools.partial(kernel, size, chunks, d**-0.5, heads),
            out_shape=pltpu.VMEM((n * per, SUB, d), q.dtype),
            in_specs=[pl.BlockSpec(memory_space=pl.ANY)] * 3,
            out_specs=pl.BlockSpec(memory_space=pltpu.VMEM),
            scratch_shapes=[
                pltpu.VMEM(q.shape, q.dtype),
                pltpu.VMEM((SLOTS, rows, d), k.dtype),
                pltpu.VMEM((SLOTS, rows, d), v.dtype),
                *[pltpu.VMEM((rows // 2, 2 * nq), jnp.float32)] * 2,
                *[pltpu.VMEM((2 * nq, rows // 2), jnp.bfloat16)] * 2,
                pltpu.VMEM((n * per, SUB, d), jnp.bfloat16),
                pltpu.VMEM((n, 1, 2 * nq), jnp.float32),
                pltpu.VMEM((2 * nq, size), jnp.float32),
                *[pltpu.VMEM((size, g * per // size, SUB, d), jnp.bfloat16) for _, g in chunks],
                *[pltpu.VMEM((size, 1, 2 * nq), jnp.float32) for _ in chunks],
                pltpu.SemaphoreType.DMA,
                pltpu.SemaphoreType.DMA((SLOTS,)),
                pltpu.SemaphoreType.DMA((SLOTS,)),
                pltpu.SemaphoreType.DMA((8, nc)),
            ],
            compiler_params=pltpu.CompilerParams(collective_id=0, has_side_effects=True, vmem_limit_bytes=60 * 1024 * 1024),
        )(q, k.reshape(n, rows, d), v.reshape(n, rows, d))
        return out.reshape(q.shape)

    return jax.shard_map(
        step,
        mesh=mesh,
        in_specs=(P("dp", None, None), P("dp", "sp", None, None), P("dp", "sp", None, None)),
        out_specs=P("dp", None, None),
        check_vma=False,
    )
```

```python
import functools

import jax
import jax.numpy as jnp
from jax import lax
from jax.experimental import pallas as pl
from jax.experimental.pallas import tpu as pltpu
from jax.sharding import PartitionSpec as P

EARLY = 3
SLOTS = 8
BLOCK = 512
CORES = 2
JOIN_LAG = 12
SUB = 8
LOG2E = 1.4426950408889634


def chunks_of(n, unit):
    sizes = [8 * unit, 4 * unit, 4 * unit]
    assert sum(sizes) == n
    return [(sum(sizes[:i]), g) for i, g in enumerate(sizes)]


def kernel(size, chunks, scale, heads, q_hbm, k_hbm, v_hbm, o_ref, q_ref, kbuf, vbuf, sb0, sb1, pb0, pb1, send, stat, cols, *rest):
    nc = len(chunks)
    recv, rstat = rest[:nc], rest[nc : 2 * nc]
    qsem, ksem, vsem, sems = rest[2 * nc :]
    sbufs, pbufs = (sb0, sb1), (pb0, pb1)
    PART_OUT, PART_IN, STAT_OUT, STAT_IN, RES_OUT, RES_IN, PASS_OUT, PASS_IN = range(8)
    n, nq, d = q_hbm.shape
    rows = k_hbm.shape[1]
    half = rows // 2
    nblk = half // BLOCK
    per = nq // SUB
    c2 = scale * LOG2E
    me = lax.axis_index("sp")
    zs = size // CORES
    core, z = lax.rem(me, CORES), me // CORES

    def spread(z):
        return lax.rem(z * (zs // 2 + 1), zs)

    def owner(j):
        return lax.rem(j, CORES) * zs + spread(j // CORES)

    def device(o):
        return spread(lax.rem(o, zs)) * CORES + o // zs

    barrier = pltpu.get_barrier_semaphore()
    for i in range(1, size):
        pl.semaphore_signal(barrier, inc=1, device_id={"sp": lax.rem(me + i, size)}, device_id_type=pl.DeviceIdType.MESH)

    def kcopy(s):
        return pltpu.make_async_copy(k_hbm.at[s], kbuf.at[lax.rem(s, SLOTS)], ksem.at[lax.rem(s, SLOTS)])

    def vcopy(s):
        return pltpu.make_async_copy(v_hbm.at[s], vbuf.at[lax.rem(s, SLOTS)], vsem.at[lax.rem(s, SLOTS)])

    qcopy = pltpu.make_async_copy(q_hbm, q_ref, qsem)
    qcopy.start()
    for s in range(EARLY):
        kcopy(s).start()
        vcopy(s).start()

    row = lax.broadcasted_iota(jnp.int32, (heads, 2 * nq), 0)
    lane = lax.broadcasted_iota(jnp.int32, (heads, 2 * nq), 1)
    keep = row == lax.rem(lane, nq) // (nq // heads)
    first = lax.broadcasted_iota(jnp.int32, (1, 2 * nq), 1) < nq

    def scores(s, b, w, m, sbuf):
        slot = lax.rem(s, SLOTS)
        k0 = kbuf[slot, pl.ds(b * BLOCK, BLOCK), :]
        k1 = kbuf[slot, pl.ds(half + b * BLOCK, BLOCK), :]
        x = lax.dot_general(jnp.concatenate([k0, k1], 1), w, (((1,), (1,)), ((), ())), preferred_element_type=jnp.float32)
        x = jnp.where(keep[None], x.reshape(BLOCK // heads, heads, 2 * nq), -jnp.inf)
        sbuf[pl.ds(b * BLOCK, BLOCK), :] = x.reshape(BLOCK, 2 * nq)
        return jnp.maximum(m, jnp.max(x, 0))

    def weights(b, mc, l, sbuf, pbuf):
        p = jnp.exp2(sbuf[pl.ds(b * BLOCK, BLOCK), :] * c2 - mc)
        pbuf[:, pl.ds(b * BLOCK, BLOCK)] = p.astype(jnp.bfloat16).T
        return l + jnp.sum(p.reshape(BLOCK // heads, heads, 2 * nq), 0)

    def values(s, b, acc, pbuf):
        slot = lax.rem(s, SLOTS)
        at = pl.ds(b * BLOCK, BLOCK)
        acc = acc + jnp.dot(pbuf[:nq, at], vbuf[slot, at, :], preferred_element_type=jnp.float32)
        return acc + jnp.dot(pbuf[nq:, at], vbuf[slot, pl.ds(half + b * BLOCK, BLOCK), :], preferred_element_type=jnp.float32)

    def fold(x, op, reduce):
        x = reduce(x, 0, keepdims=True)
        return op(x, pltpu.roll(x, nq, 1))

    def stat_of(m, l):
        return jnp.where(first, m, fold(l, jnp.add, jnp.sum))

    def stage(s, side, state, which):
        m8, l8, m2 = state
        m = jnp.full((heads, 2 * nq), -jnp.inf, jnp.float32)
        l = jnp.zeros((heads, 2 * nq), jnp.float32)
        acc = jnp.zeros((nq, d), jnp.float32)
        if "A" in which:
            q = q_ref[s]
            zero = jnp.zeros_like(q)
            w = jnp.concatenate([jnp.concatenate([q, zero], 1), jnp.concatenate([zero, q], 1)], 0)
        m1 = fold(m8, jnp.maximum, jnp.max)
        for b in range(nblk):
            if "C" in which:
                acc = values(s - 2, b, acc, pbufs[side])
            if "B" in which:
                l = weights(b, m1 * c2, l, sbufs[1 - side], pbufs[1 - side])
            if "A" in which:
                m = scores(s, b, w, m, sbufs[side])
        if "C" in which:
            send[pl.ds((s - 2) * per, per)] = acc.reshape(per, SUB, d).astype(send.dtype)
            if "B" in which:
                stat[s - 2] = stat_of(m2, l8)
        return m, l, m1

    def shape_of(c):
        base, g = chunks[c]
        r = g * per // size
        return base, g, r

    def rows_of(c, o):
        base, _, r = shape_of(c)
        return pl.ds(base * per + o * r, r)

    def seq_of(c, o):
        base, _, r = shape_of(c)
        return base + (o * r) // per

    def remote(src, dst, out, into, j):
        return pltpu.make_async_remote_copy(src, dst, out, into, device_id={"sp": j}, device_id_type=pl.DeviceIdType.MESH)

    def wait_for(ref, sem):
        pltpu.make_async_copy(ref, ref, sem).wait()

    def peers():
        for i in [x for k in range(zs // 2) for x in (zs // 2 - k, zs // 2 + k)[: 1 + (k > 0)]]:
            for k in range(CORES):
                yield lax.rem(z + i, zs) * CORES + lax.rem(core + k, CORES)
        for k in range(1, CORES):
            yield z * CORES + lax.rem(core + k, CORES)

    def owners_of(c, s):
        base, _, r = shape_of(c)
        return [(s - base) * (per // r) + i for i in range(per // r)]

    def to_owners(c, s, part=True, stats=True):
        for o in owners_of(c, s):
            j = device(o)

            @pl.when(j != me)
            def _():
                if stats:
                    remote(stat.at[s], rstat[c].at[me], sems.at[STAT_OUT, c], sems.at[STAT_IN, c], j).start()
                if part:
                    remote(send.at[rows_of(c, o)], recv[c].at[me], sems.at[PART_OUT, c], sems.at[PART_IN, c], j).start()

    def combine(c, direct):
        base, g, r = shape_of(c)
        o = owner(me)
        rstat[c][me] = stat[seq_of(c, o)]
        wait_for(rstat[c].at[pl.ds(0, size - 1)], sems.at[STAT_IN, c])
        st = rstat[c][...].reshape(size, 2 * nq)
        e = jnp.exp2((st - jnp.max(st, 0, keepdims=True)) * c2)
        f = e / jnp.sum(e * pltpu.roll(st, nq, 1), 0, keepdims=True)
        cols[...] = f.T
        f = cols[pl.ds(pl.multiple_of(lax.rem(o * r, per) * SUB, SUB), r * SUB), :]
        recv[c][me] = send[rows_of(c, o)]
        wait_for(recv[c].at[pl.ds(0, size - 1)], sems.at[PART_IN, c])
        acc = jnp.zeros((r * SUB, d), jnp.float32)
        for j in range(size):
            acc = acc + recv[c][j].astype(jnp.float32).reshape(r * SUB, d) * f[:, j : j + 1]
        mine = rows_of(c, o)
        o_ref[mine] = acc.reshape(r, SUB, d).astype(o_ref.dtype)
        for i, j in enumerate(peers()):
            if direct or i % CORES == 0 and i < (zs - 1) * CORES:
                remote(o_ref.at[mine], o_ref.at[mine], sems.at[RES_OUT, c], sems.at[RES_IN, c], j).start()

    def count(c, k):
        return o_ref.at[pl.ds(0, k * shape_of(c)[2])]

    def pass_on(c):
        base, g, r = shape_of(c)
        wait_for(count(c, zs - 1), sems.at[RES_IN, c])
        own = o_ref.at[pl.ds(base * per + core * zs * r, zs * r)]
        remote(own, own, sems.at[PASS_OUT, c], sems.at[PASS_IN, c], z * CORES + lax.rem(core + 1, CORES)).start()

    last = nc - 1
    assert chunks[0][1] == size and size + JOIN_LAG <= n - 4

    state = (jnp.zeros((heads, 2 * nq), jnp.float32), jnp.zeros((heads, 2 * nq), jnp.float32), jnp.zeros((1, 2 * nq), jnp.float32))

    def refill(copy, s):
        @pl.when(s + SLOTS < n)
        def _():
            copy(s + SLOTS).start()

    qcopy.wait()
    kcopy(0).wait()
    for s in range(EARLY, SLOTS):
        kcopy(s).start()
        vcopy(s).start()
    state = stage(0, 0, state, "A")
    refill(kcopy, 0)
    kcopy(1).wait()
    state = stage(1, 1, state, "BA")
    refill(kcopy, 1)

    def body(c, i, state):
        s = 2 * i
        for u in range(2):
            kcopy(s + u).wait()
            vcopy(s + u - 2).wait()
        for u in range(2):
            state = stage(s + u, u, state, "ABC")
        for u in range(2):
            refill(kcopy, s + u)
            refill(vcopy, s + u - 2)
        for u in range(2):
            to_owners(c, s + u - 2)

        @pl.when(owner(me) // 2 == i - 1 - JOIN_LAG // 2)
        def _():
            combine(0, False)

        return state

    pl.semaphore_wait(barrier, size - 1)
    for c, (base, g) in enumerate(chunks):
        lo, hi = base, min(base + g, n - 4)
        if lo < hi:
            state = lax.fori_loop(lo // 2 + 1, hi // 2 + 1, functools.partial(body, c), state)
    for s in (n - 2, n - 1):
        kcopy(s).wait()
        vcopy(s - 2).wait()
        state = stage(s, s % 2, state, "ABC")
        to_owners(last, s - 2)
    vcopy(n - 2).wait()
    m8, l8, m2 = stage(n, 0, state, "BC")
    stat[n - 1] = stat_of(m2, l8)
    to_owners(last, n - 2)
    to_owners(last, n - 1, part=False)
    vcopy(n - 1).wait()
    stage(n + 1, 1, (m8, l8, m2), "C")
    to_owners(last, n - 1, stats=False)
    for c in range(1, last):
        combine(c, False)
    pass_on(0)
    combine(last, True)
    for c in range(1, last):
        pass_on(c)
    for c in range(last):
        base, g, r = shape_of(c)
        wait_for(count(c, zs), sems.at[PASS_IN, c])
    wait_for(count(last, size - 1), sems.at[RES_IN, last])
    for c in range(nc):
        wait_for(recv[c].at[pl.ds(0, size - 1)], sems.at[PART_OUT, c])
        wait_for(rstat[c].at[pl.ds(0, size - 1)], sems.at[STAT_OUT, c])
        wait_for(count(c, size - 1 if c == last else zs - 1), sems.at[RES_OUT, c])
        if c < last:
            wait_for(count(c, zs), sems.at[PASS_OUT, c])


def solution(mesh):
    size = mesh.shape["sp"]

    def step(q, k, v):
        n, nq, d = q.shape
        t, heads = k.shape[1:3]
        per = nq // SUB
        chunks = chunks_of(n, size // per)
        nc = len(chunks)
        rows = t * heads
        out = pl.pallas_call(
            functools.partial(kernel, size, chunks, d**-0.5, heads),
            out_shape=pltpu.VMEM((n * per, SUB, d), q.dtype),
            in_specs=[pl.BlockSpec(memory_space=pl.ANY)] * 3,
            out_specs=pl.BlockSpec(memory_space=pltpu.VMEM),
            scratch_shapes=[
                pltpu.VMEM(q.shape, q.dtype),
                pltpu.VMEM((SLOTS, rows, d), k.dtype),
                pltpu.VMEM((SLOTS, rows, d), v.dtype),
                *[pltpu.VMEM((rows // 2, 2 * nq), jnp.float32)] * 2,
                *[pltpu.VMEM((2 * nq, rows // 2), jnp.bfloat16)] * 2,
                pltpu.VMEM((n * per, SUB, d), jnp.bfloat16),
                pltpu.VMEM((n, 1, 2 * nq), jnp.float32),
                pltpu.VMEM((2 * nq, size), jnp.float32),
                *[pltpu.VMEM((size, g * per // size, SUB, d), jnp.bfloat16) for _, g in chunks],
                *[pltpu.VMEM((size, 1, 2 * nq), jnp.float32) for _ in chunks],
                pltpu.SemaphoreType.DMA,
                pltpu.SemaphoreType.DMA((SLOTS,)),
                pltpu.SemaphoreType.DMA((SLOTS,)),
                pltpu.SemaphoreType.DMA((8, nc)),
            ],
            compiler_params=pltpu.CompilerParams(collective_id=0, has_side_effects=True, vmem_limit_bytes=60 * 1024 * 1024),
        )(q, k.reshape(n, rows, d), v.reshape(n, rows, d))
        return out.reshape(q.shape)

    return jax.shard_map(
        step,
        mesh=mesh,
        in_specs=(P("dp", None, None), P("dp", "sp", None, None), P("dp", "sp", None, None)),
        out_specs=P("dp", None, None),
        check_vma=False,
    )
```
